128 devices in a mesh: row: 8 (over x, y_hi), col: 16 (over z, y_lo, core).
Axes of the slice: x: 4, y: 4 (y_hi: 2, y_lo: 2; y = y_hi * 2 + y_lo), z: 4, core: 2. Of those that a mesh axis runs over, the one named last changes fastest.
Arguments:
- voltages: bfloat16 [4096, 64, 2, 256], P(('col', 'row')), may hold values from -6 to 6
- auto_prev: float32 [64, 4096], P('row', 'col'), may hold values from 0.5 to 8
- station_order: int32 [4096], replicated, may hold values from 0 to 4095, each once
Outputs:
- visibilities: bfloat16 [64, 9, 4096, 512], P('row', None, 'col')
The draws below stay inside these ranges and needn't reach their ends.
Inputs may be any that keep to these rules, and one draw needn't show every extreme that they name: `station_order`: a permutation of the block positions.
All inputs are finite; a program needn't handle non-finite values.
Results may differ from the reference program's by a relative error of at most 0.001.
Values may be sent and summed in bfloat16 or wider, within the bound.
A program may use at most 128 MiB of HBM per device.

```python
import math
import jax
import jax.numpy as jnp
from jax import lax

STATIONS = 4096
SAMPLES = 256
CHANNELS = 64
N_COL = 16


def level_of(own_key, dims, cuts, least, top_value):
    loudness, own = 1.0, jax.random.fold_in(own_key, 6)
    for axis_at, parts in cuts:
        steps = jnp.exp(jax.random.uniform(jax.random.fold_in(own, axis_at), (parts,), jnp.float32, least / len(cuts), top_value / len(cuts)))
        loudness = loudness * jnp.repeat(steps, dims[axis_at] // parts).reshape([-1 if axis == axis_at else 1 for axis in range(len(dims))])
    return loudness


def gaussian(stream_key, dims, width, bound, cuts=(), held_as=jnp.bfloat16):
    result = jax.random.normal(stream_key, dims, jnp.float32) * width
    if len(cuts) > 0:
        result = level_of(stream_key, dims, cuts, -0.22, 0.18) * result
    return jnp.clip(result, min=-bound, max=bound).astype(held_as)


def setup_inputs(seed: int = 0) -> dict:
    splits = jax.random.split(jax.random.key(seed), 4)
    voltages = gaussian(splits[0], (STATIONS, CHANNELS, 2, SAMPLES), 1.0, 6.0, ((0, 128),))
    auto_prev = jnp.clip(jnp.exp(math.log(8.0) - 2.7725887 * jax.random.uniform(splits[1], (CHANNELS, STATIONS), jnp.float32) ** level_of(splits[1], (CHANNELS, STATIONS), ((0, 8), (1, 16)), -0.2, 0.2)), 0.5, 8.0)
    station_order = jax.random.permutation(splits[2], STATIONS).astype(jnp.int32)
    return {"voltages": voltages, "auto_prev": auto_prev, "station_order": station_order}


def reference(voltages, auto_prev, station_order):
    block_size = STATIONS // N_COL
    offsets = N_COL // 2 + 1
    flat = voltages.reshape(STATIONS, CHANNELS, 2 * SAMPLES)
    turned = jnp.concatenate([-voltages[:, :, 1], voltages[:, :, 0]], axis=-1)
    inverse = 1.0 / jnp.sqrt(auto_prev[:, station_order])

    def one_block(block_index):
        first = (block_index * block_size).astype(jnp.int32)
        own_rows = lax.dynamic_slice_in_dim(flat, first, block_size, 0).astype(jnp.float32)
        row_scale = lax.dynamic_slice_in_dim(inverse, first, block_size, 1)
        tiles = []
        for offset in range(offsets):
            start = ((block_index - offset) % N_COL * block_size).astype(jnp.int32)
            partner = jnp.concatenate([lax.dynamic_slice_in_dim(flat, start, block_size, 0), lax.dynamic_slice_in_dim(turned, start, block_size, 0)], axis=0).astype(jnp.float32)
            gram = jnp.einsum('ich,jch->cij', own_rows, partner)
            column_scale = lax.dynamic_slice_in_dim(inverse, start, block_size, 1)
            column_scale = jnp.concatenate([column_scale, column_scale], axis=-1)
            tiles.append(gram * row_scale[:, :, None] * column_scale[:, None, :] * (1.0 / SAMPLES))
        return jnp.stack(tiles, axis=1).astype(jnp.bfloat16)
    blocks = lax.map(one_block, jnp.arange(N_COL, dtype=jnp.int32))
    blocks = jnp.transpose(blocks, (1, 2, 0, 3, 4))
    return blocks.reshape(CHANNELS, offsets, STATIONS, 2 * block_size)
```

```python
import functools

import jax
import jax.numpy as jnp
from jax import lax
from jax.experimental import pallas as pl
from jax.experimental.pallas import tpu as pltpu
from jax.sharding import PartitionSpec as P

CHAN = 8
HALF = CHAN // 2
PIECE = 32
BLOCK = 256
WIDE = 512
COLS = 16
TURNED_DOWN = (0, 1)


def comm_kernel(
    x, auto, order, grid, inv, inv_t,
    transit, relay, autos,
    bar_local, s_a2a, s_relay, s_half, s_z, s_y, s_die, s_auto, s_inv,
    r_x, r_o, r_rel, r_blk, r_trans, r_die, r_auto, r_inv,
):
    row = lax.axis_index("row")
    col = lax.axis_index("col")
    xpos, yhi = row // 2, row % 2
    core, ylo = col % 2, (col // 2) % 2
    sib = col + 1 - 2 * core
    ynb = col + 2 - 4 * ylo
    up = (col + 4) % COLS
    down = (col + COLS - 4) % COLS
    is0, is1 = ylo == 0, ylo == 1
    other = 1 - yhi

    def peer_x(d):
        return ((xpos + d) % 4) * 2 + yhi

    def peer_o(d):
        return ((xpos + d) % 4) * 2 + other

    def remote(src, dst, ss, rs, **where):
        return pltpu.make_async_remote_copy(
            src_ref=src, dst_ref=dst, send_sem=ss, recv_sem=rs,
            device_id=where, device_id_type=pl.DeviceIdType.MESH,
        )

    barrier = pltpu.get_barrier_semaphore()
    for d in range(1, 4):
        pl.semaphore_signal(barrier, inc=1, device_id={"row": peer_x(d), "col": col}, device_id_type=pl.DeviceIdType.MESH)
    for d in range(4):
        pl.semaphore_signal(barrier, inc=1, device_id={"row": peer_o(d), "col": ynb}, device_id_type=pl.DeviceIdType.MESH)
    for d in range(1, COLS):
        pl.semaphore_signal(barrier, inc=1, device_id={"row": row, "col": (col + d) % COLS}, device_id_type=pl.DeviceIdType.MESH)
    pl.semaphore_wait(barrier, 3 + 4 + COLS - 1)

    def local_own(ch):
        return pltpu.make_async_copy(x.at[row * CHAN + ch], grid.at[0, ch, xpos, yhi], bar_local.at[ch])

    def a2a_x(ch, d):
        return remote(x.at[peer_x(d) * CHAN + ch], grid.at[0, ch, xpos, yhi], s_a2a.at[ch], r_x.at[ch],
                      row=peer_x(d), col=col)

    def a2a_o(ch, d, first):
        dst = grid.at[2, ch, xpos, yhi] if first else relay.at[ch, xpos]
        return remote(x.at[peer_o(d) * CHAN + ch], dst, s_a2a.at[ch], r_o.at[ch], row=peer_o(d), col=ynb)

    def relayed(ch, first):
        src = relay.at[ch] if first else grid.at[2, ch, :, other]
        return remote(src, grid.at[0, ch, :, other], s_relay.at[ch], r_rel.at[ch], row=row, col=ynb)

    def half(ch):
        return remote(grid.at[0, ch, :, yhi], grid.at[2, ch, :, yhi], s_half.at[ch], r_blk.at[0, ch], row=row, col=ynb)

    def z_send(ch, j, to, target, slot):
        src = transit.at[ch] if j == 6 else grid.at[2 * j, ch]
        if to == 6:
            return remote(src, transit.at[ch], s_z.at[slot, ch], r_trans.at[ch], row=row, col=target)
        return remote(src, grid.at[2 * to, ch], s_z.at[slot, ch], r_blk.at[to - 1, ch], row=row, col=target)

    def y_send(ch, j, to, slot):
        return remote(grid.at[2 * j, ch], grid.at[2 * to, ch], s_y.at[slot, ch], r_blk.at[to - 1, ch], row=row, col=ynb)

    def die(ch, j):
        at = j - core
        return remote(grid.at[2 * j, ch], grid.at[2 * at + 1, ch], s_die.at[at, ch], r_die.at[at, ch], row=row, col=sib)

    def die_start(ch, j):
        if j == 0:
            pl.when(core == 0)(lambda: die(ch, j).start())
        elif j == 4:
            pl.when(core == 1)(lambda: die(ch, j).start())
        else:
            die(ch, j).start()

    def got(sem, ref):
        pltpu.make_async_copy(ref, ref, sem).wait()

    def got_block(j, ch):
        got(r_blk.at[j - 1, ch], grid.at[2 * j, ch])

    def each(count, body):
        lax.fori_loop(0, count, lambda i, carry: (body(i), carry)[1], 0)

    def send_auto(d):
        return remote(auto, autos.at[col], s_auto, r_auto, row=row, col=(col + d) % COLS)

    def exchange(ch):
        local_own(ch).start()
        for d in range(1, 4):
            a2a_x(ch, d).start()
        for d in range(4):
            pl.when(is0)(lambda: a2a_o(ch, d, True).start())
            pl.when(is1)(lambda: a2a_o(ch, d, False).start())

    exchange(0)
    exchange(HALF)
    each(COLS - 1, lambda i: send_auto(i + 1).start())
    autos[pl.ds(col, 1)] = auto[...][None]

    def exchange_pair(i):
        exchange(i + 1)
        exchange(i + 1 + HALF)

    each(HALF - 1, exchange_pair)

    def ready_half(ch):
        got(r_o.at[ch], relay.at[ch])
        pl.when(is0)(lambda: relayed(ch, True).start())
        pl.when(is1)(lambda: relayed(ch, False).start())
        local_own(ch).wait()
        got(r_x.at[ch], x.at[pl.ds(0, 3)])
        pl.when(is0)(lambda: half(ch).start())

    def ready_own_down(ch):
        got(r_rel.at[ch], relay.at[ch])
        z_send(ch, 0, 6, down, 0).start()
        die_start(ch, 0)

    def ready_own_up(ch):
        got(r_rel.at[ch], relay.at[ch])
        z_send(ch, 0, 2, up, 0).start()
        die_start(ch, 0)

    ready_half(0)
    ready_half(HALF)

    def own_pair(i):
        ready_half(i + 1)
        ready_own_down(i)
        ready_half(i + 1 + HALF)
        ready_own_up(i + HALF)

    each(HALF - 1, own_pair)
    ready_own_down(HALF - 1)
    ready_own_up(CHAN - 1)

    got(r_auto, autos.at[pl.ds(0, COLS - 1)])
    mine = order[pl.ds(col, 1), :]

    def gathered(b, total):
        values = autos[pl.ds(b, 1)].reshape(CHAN, BLOCK)
        high = values.astype(jnp.bfloat16)
        rest = values - high.astype(jnp.float32)
        mid = rest.astype(jnp.bfloat16)
        low = (rest - mid.astype(jnp.float32)).astype(jnp.bfloat16)
        stations = lax.broadcasted_iota(jnp.int32, (BLOCK, BLOCK), 0) + b * BLOCK
        hot = jnp.where(stations == mine, 1.0, 0.0).astype(jnp.bfloat16)
        for part in (low, mid, high):
            total = total + jnp.dot(part, hot, preferred_element_type=jnp.float32)
        return total

    values = lax.fori_loop(0, COLS, gathered, jnp.zeros((CHAN, BLOCK), jnp.float32))
    inverse = 1.0 / jnp.sqrt(values)
    inv[0] = inverse
    inv_t[...] = jnp.transpose(inverse)

    def second(i):
        ch = i + HALF
        got(r_trans.at[i], transit.at[i])
        z_send(i, 6, 4, down, 1).start()
        got_block(2, ch)
        z_send(ch, 2, 4, up, 1).start()
        pl.when(is1)(lambda: y_send(ch, 2, 1, 0).start())
        die_start(ch, 2)

        @pl.when(is1)
        def _():
            got(r_blk.at[0, ch], relay.at[ch])
            z_send(ch, 1, 3, up, 2).start()
            die_start(ch, 1)

    each(HALF, second)

    def send_inv(k):
        return remote(inv.at[0], inv.at[k], s_inv, r_inv, row=row, col=(col + k) % COLS)

    for k in range(1, 9):
        send_inv(k).start()

    def third(i):
        ch = i + HALF
        got_block(4, i)
        z_send(i, 4, 2, down, 2).start()
        pl.when(is1)(lambda: y_send(i, 4, 3, 0).start())
        die_start(i, 4)

        @pl.when(is0)
        def _():
            got_block(1, ch)
            z_send(ch, 1, 3, up, 2).start()
            die_start(ch, 1)

        @pl.when(is1)
        def _():
            got(r_blk.at[0, i], relay.at[i])
            die_start(i, 1)

    each(HALF, third)

    def turned_down(i):
        return i < len(TURNED_DOWN)

    def turn(i):
        @pl.when(is0)
        def _():
            got_block(3, i)
            z_send(i, 3, 1, down, 3).start()
            die_start(i, 3)

    each(len(TURNED_DOWN), turn)

    def fourth(i):
        ch = i + HALF
        got_block(2, i)
        pl.when(is0)(lambda: y_send(i, 2, 3, 1).start())
        pl.when(jnp.logical_and(is1, i >= len(TURNED_DOWN)))(lambda: y_send(i, 2, 1, 1).start())
        die_start(i, 2)
        got_block(4, ch)
        die_start(ch, 4)
        got_block(3, ch)
        die_start(ch, 3)

    each(HALF, fourth)

    def last(i):
        @pl.when(is0)
        def _():
            @pl.when(i >= len(TURNED_DOWN))
            def _():
                got_block(3, i)
                die_start(i, 3)
            got_block(1, i)
            die_start(i, 1)

        @pl.when(is1)
        def _():
            got_block(3, i)
            die_start(i, 3)

    each(HALF, last)

    def settle(ch):
        got(s_a2a.at[ch], x.at[pl.ds(0, 7)])
        relayed(ch, True).wait_send()
        pl.when(is0)(lambda: half(ch).wait_send())
        for at in range(4):
            got(r_die.at[at, ch], grid.at[2 * at + 1, ch])
            got(s_die.at[at, ch], grid.at[2 * at + 1, ch])
        for slot in range(3):
            got(s_z.at[slot, ch], grid.at[0, ch])

    each(CHAN, settle)

    def settle_down(i):
        @pl.when(is0)
        def _():
            got(s_y.at[1, i], grid.at[0, i])
            pl.when(turned_down(i))(lambda: got(s_z.at[3, i], grid.at[0, i]))

        @pl.when(is1)
        def _():
            got(s_y.at[0, i], grid.at[0, i])
            got(s_y.at[0, i + HALF], grid.at[0, i])
            pl.when(i >= len(TURNED_DOWN))(lambda: got(s_y.at[1, i], grid.at[0, i]))

    each(HALF, settle_down)
    got(s_auto, autos.at[pl.ds(0, COLS - 1)])
    got(s_inv, inv.at[pl.ds(1, 8)])
    got(r_inv, inv.at[pl.ds(1, 8)])


def tile_kernel(grid, inv, inv_t, out):
    h = pl.program_id(0)
    own = grid[0, 0]
    turned = jnp.concatenate([own[:, BLOCK:], -own[:, :BLOCK]], axis=1)
    lanes = lax.broadcasted_iota(jnp.int32, (BLOCK, CHAN), 1)
    rows = jnp.sum(jnp.where(lanes == h, inv_t[...], 0.0), axis=1, keepdims=True) * (1.0 / BLOCK)
    for k in range(9):
        partner = grid[k, 0]
        factor = rows * inv[k, pl.ds(h, 1), :]
        for half, left in enumerate((own, turned)):
            gram = lax.dot_general(left, partner, (((1,), (1,)), ((), ())), preferred_element_type=jnp.float32)
            out[0, k, :, half * BLOCK:(half + 1) * BLOCK] = (gram * factor).astype(jnp.bfloat16)


def per_device(voltages, auto_prev, station_order):
    x = jnp.transpose(voltages.reshape(PIECE, 64, WIDE), (1, 0, 2))
    order = station_order.reshape(COLS, BLOCK)
    any_space = pl.BlockSpec(memory_space=pl.ANY)
    vmem = pl.BlockSpec(memory_space=pltpu.VMEM)
    dma = pltpu.SemaphoreType.DMA
    grid, inv, inv_t = pl.pallas_call(
        comm_kernel,
        out_shape=(
            jax.ShapeDtypeStruct((9, CHAN, 4, 2, PIECE, WIDE), jnp.bfloat16),
            jax.ShapeDtypeStruct((9, CHAN, BLOCK), jnp.float32),
            jax.ShapeDtypeStruct((BLOCK, CHAN), jnp.float32),
        ),
        in_specs=[any_space, vmem, vmem],
        out_specs=(any_space, vmem, vmem),
        scratch_shapes=[
            pltpu.VMEM((HALF, 4, 2, PIECE, WIDE), jnp.bfloat16),
            pltpu.VMEM((CHAN, 4, PIECE, WIDE), jnp.bfloat16),
            pltpu.VMEM((COLS, CHAN, BLOCK), jnp.float32),
            dma((CHAN,)), dma((CHAN,)), dma((CHAN,)), dma((CHAN,)), dma((4, CHAN)), dma((2, CHAN)), dma((4, CHAN)), dma, dma,
            dma((CHAN,)), dma((CHAN,)), dma((CHAN,)), dma((4, CHAN)), dma((HALF,)), dma((4, CHAN)), dma, dma,
        ],
        compiler_params=pltpu.CompilerParams(collective_id=0, has_side_effects=True),
    )(x, auto_prev, order)
    grid = grid.reshape(9, CHAN, BLOCK, WIDE)
    return pl.pallas_call(
        tile_kernel,
        grid=(CHAN,),
        out_shape=jax.ShapeDtypeStruct((CHAN, 9, BLOCK, WIDE), jnp.bfloat16),
        in_specs=[
            pl.BlockSpec((9, 1, BLOCK, WIDE), lambda h: (0, h, 0, 0)),
            vmem,
            vmem,
        ],
        out_specs=pl.BlockSpec((1, 9, BLOCK, WIDE), lambda h: (h, 0, 0, 0)),
    )(grid, inv, inv_t)


def solution(mesh):
    return jax.shard_map(
        per_device,
        mesh=mesh,
        in_specs=(P(("col", "row"), None, None, None), P("row", "col"), P()),
        out_specs=P("row", None, "col", None),
        check_vma=False,
    )
```

```python
import functools

import jax
import jax.numpy as jnp
from jax import lax
from jax.experimental import pallas as pl
from jax.experimental.pallas import tpu as pltpu
from jax.sharding import PartitionSpec as P

CHAN = 8
HALF = CHAN // 2
PIECE = 32
BLOCK = 256
WIDE = 512
COLS = 16
LAG = 2
TURNED_DOWN = (0, 1)


def comm_kernel(
    x, auto, order, grid, inv, inv_t,
    transit, relay, autos,
    bar_local, s_a2a, s_relay, s_half, s_z, s_y, s_die, s_auto, s_inv,
    r_x, r_o, r_rel, r_blk, r_trans, r_die, r_auto, r_inv,
):
    row = lax.axis_index("row")
    col = lax.axis_index("col")
    xpos, yhi = row // 2, row % 2
    core, ylo = col % 2, (col // 2) % 2
    sib = col + 1 - 2 * core
    ynb = col + 2 - 4 * ylo
    up = (col + 4) % COLS
    down = (col + COLS - 4) % COLS
    is0, is1 = ylo == 0, ylo == 1
    other = 1 - yhi

    def peer_x(d):
        return ((xpos + d) % 4) * 2 + yhi

    def peer_o(d):
        return ((xpos + d) % 4) * 2 + other

    def remote(src, dst, ss, rs, **where):
        return pltpu.make_async_remote_copy(
            src_ref=src, dst_ref=dst, send_sem=ss, recv_sem=rs,
            device_id=where, device_id_type=pl.DeviceIdType.MESH,
        )

    barrier = pltpu.get_barrier_semaphore()
    for d in range(1, 4):
        pl.semaphore_signal(barrier, inc=1, device_id={"row": peer_x(d), "col": col}, device_id_type=pl.DeviceIdType.MESH)
    for d in range(4):
        pl.semaphore_signal(barrier, inc=1, device_id={"row": peer_o(d), "col": ynb}, device_id_type=pl.DeviceIdType.MESH)
    for d in range(1, COLS):
        pl.semaphore_signal(barrier, inc=1, device_id={"row": row, "col": (col + d) % COLS}, device_id_type=pl.DeviceIdType.MESH)
    pl.semaphore_wait(barrier, 3 + 4 + COLS - 1)

    def local_own(ch):
        return pltpu.make_async_copy(x.at[row * CHAN + ch], grid.at[0, ch, xpos, yhi], bar_local.at[ch])

    def a2a_x(ch, d):
        return remote(x.at[peer_x(d) * CHAN + ch], grid.at[0, ch, xpos, yhi], s_a2a.at[ch], r_x.at[ch],
                      row=peer_x(d), col=col)

    def a2a_o(ch, d, first):
        dst = grid.at[2, ch, xpos, yhi] if first else relay.at[ch, xpos]
        return remote(x.at[peer_o(d) * CHAN + ch], dst, s_a2a.at[ch], r_o.at[ch], row=peer_o(d), col=ynb)

    def relayed(ch, first):
        src = relay.at[ch] if first else grid.at[2, ch, :, other]
        return remote(src, grid.at[0, ch, :, other], s_relay.at[ch], r_rel.at[ch], row=row, col=ynb)

    def half(ch):
        return remote(grid.at[0, ch, :, yhi], grid.at[2, ch, :, yhi], s_half.at[ch], r_blk.at[0, ch], row=row, col=ynb)

    def z_send(ch, j, to, target, slot):
        src = transit.at[ch] if j == 6 else grid.at[2 * j, ch]
        if to == 6:
            return remote(src, transit.at[ch], s_z.at[slot, ch], r_trans.at[ch], row=row, col=target)
        return remote(src, grid.at[2 * to, ch], s_z.at[slot, ch], r_blk.at[to - 1, ch], row=row, col=target)

    def y_send(ch, j, to, slot):
        return remote(grid.at[2 * j, ch], grid.at[2 * to, ch], s_y.at[slot, ch], r_blk.at[to - 1, ch], row=row, col=ynb)

    def die(ch, j):
        at = j - core
        return remote(grid.at[2 * j, ch], grid.at[2 * at + 1, ch], s_die.at[at, ch], r_die.at[at, ch], row=row, col=sib)

    def die_start(ch, j):
        if j == 0:
            pl.when(core == 0)(lambda: die(ch, j).start())
        elif j == 4:
            pl.when(core == 1)(lambda: die(ch, j).start())
        else:
            die(ch, j).start()

    def got(sem, ref):
        pltpu.make_async_copy(ref, ref, sem).wait()

    def got_block(j, ch):
        got(r_blk.at[j - 1, ch], grid.at[2 * j, ch])

    def each(count, body):
        lax.fori_loop(0, count, lambda i, carry: (body(i), carry)[1], 0)

    def send_auto(d):
        return remote(auto, autos.at[col], s_auto, r_auto, row=row, col=(col + d) % COLS)

    def exchange(ch):
        local_own(ch).start()
        for d in range(1, 4):
            a2a_x(ch, d).start()
        for d in range(4):
            pl.when(is0)(lambda: a2a_o(ch, d, True).start())
            pl.when(is1)(lambda: a2a_o(ch, d, False).start())

    exchange(0)
    exchange(HALF)
    each(COLS - 1, lambda i: send_auto(i + 1).start())
    autos[pl.ds(col, 1)] = auto[...][None]

    def exchange_pair(i):
        exchange(i + 1)
        exchange(i + 1 + HALF)

    each(HALF - 1, exchange_pair)

    def own_z(ch, part, falls):
        src = grid.at[0, ch, :, part]
        if falls:
            return remote(src, transit.at[ch, :, part], s_z.at[0, ch], r_trans.at[ch], row=row, col=down)
        return remote(src, grid.at[4, ch, :, part], s_z.at[0, ch], r_blk.at[1, ch], row=row, col=up)

    def ready_half(ch, falls):
        got(r_o.at[ch], relay.at[ch])
        pl.when(is0)(lambda: relayed(ch, True).start())
        pl.when(is1)(lambda: relayed(ch, False).start())
        local_own(ch).wait()
        got(r_x.at[ch], x.at[pl.ds(0, 3)])
        own_z(ch, yhi, falls).start()

    def ready_own(ch, falls):
        got(r_rel.at[ch], relay.at[ch])
        own_z(ch, other, falls).start()
        die_start(ch, 0)

    def second_down(i):
        got(r_trans.at[i], transit.at[i])
        z_send(i, 6, 4, down, 1).start()

    def second_up(ch):
        got_block(2, ch)
        z_send(ch, 2, 4, up, 1).start()
        pl.when(is1)(lambda: y_send(ch, 2, 1, 0).start())
        die_start(ch, 2)

    def step(i):
        if i < HALF:
            ready_half(i, True)
        if 0 <= i - 1 < HALF:
            ready_own(i - 1, True)
        if i < HALF:
            ready_half(i + HALF, False)
        if 0 <= i - 1 < HALF:
            ready_own(i - 1 + HALF, False)
        if 0 <= i - LAG < HALF:
            second_down(i - LAG)
            second_up(i - LAG + HALF)

    for i in range(HALF + 1):
        step(i)

    @pl.when(is0)
    def _():
        each(HALF, lambda i: half(i + HALF).start())
        each(HALF, lambda i: half(i).start())

    got(r_auto, autos.at[pl.ds(0, COLS - 1)])
    mine = order[pl.ds(col, 1), :]

    def gathered(b, total):
        values = autos[pl.ds(b, 1)].reshape(CHAN, BLOCK)
        high = values.astype(jnp.bfloat16)
        rest = values - high.astype(jnp.float32)
        mid = rest.astype(jnp.bfloat16)
        low = (rest - mid.astype(jnp.float32)).astype(jnp.bfloat16)
        stations = lax.broadcasted_iota(jnp.int32, (BLOCK, BLOCK), 0) + b * BLOCK
        hot = jnp.where(stations == mine, 1.0, 0.0).astype(jnp.bfloat16)
        for part in (low, mid, high):
            total = total + jnp.dot(part, hot, preferred_element_type=jnp.float32)
        return total

    values = lax.fori_loop(0, COLS, gathered, jnp.zeros((CHAN, BLOCK), jnp.float32))
    inverse = 1.0 / jnp.sqrt(values)
    inv[0] = inverse
    inv_t[...] = jnp.transpose(inverse)

    for i in range(HALF + 1, HALF + LAG):
        step(i)

    @pl.when(is1)
    def _():
        def early(i):
            ch = i + HALF
            got(r_blk.at[0, ch], relay.at[ch])
            z_send(ch, 1, 3, up, 2).start()
            die_start(ch, 1)
        each(HALF, early)

    def send_inv(k):
        return remote(inv.at[0], inv.at[k], s_inv, r_inv, row=row, col=(col + k) % COLS)

    for k in range(1, 9):
        send_inv(k).start()

    def third(i):
        ch = i + HALF
        got_block(4, i)
        z_send(i, 4, 2, down, 2).start()
        pl.when(is1)(lambda: y_send(i, 4, 3, 0).start())
        die_start(i, 4)

        @pl.when(is0)
        def _():
            got_block(1, ch)
            z_send(ch, 1, 3, up, 2).start()
            die_start(ch, 1)

        @pl.when(is1)
        def _():
            got(r_blk.at[0, i], relay.at[i])
            die_start(i, 1)

    each(HALF, third)

    def turned_down(i):
        return i < len(TURNED_DOWN)

    def turn(i):
        @pl.when(is0)
        def _():
            got_block(3, i)
            z_send(i, 3, 1, down, 3).start()
            die_start(i, 3)

    each(len(TURNED_DOWN), turn)

    def fourth(i):
        ch = i + HALF
        got_block(2, i)
        pl.when(is0)(lambda: y_send(i, 2, 3, 1).start())
        pl.when(jnp.logical_and(is1, i >= len(TURNED_DOWN)))(lambda: y_send(i, 2, 1, 1).start())
        die_start(i, 2)
        got_block(4, ch)
        die_start(ch, 4)
        got_block(3, ch)
        die_start(ch, 3)

    each(HALF, fourth)

    def last(i):
        @pl.when(is0)
        def _():
            @pl.when(i >= len(TURNED_DOWN))
            def _():
                got_block(3, i)
                die_start(i, 3)
            got_block(1, i)
            die_start(i, 1)

        @pl.when(is1)
        def _():
            got_block(3, i)
            die_start(i, 3)

    each(HALF, last)

    def settle(ch):
        got(s_a2a.at[ch], x.at[pl.ds(0, 7)])
        relayed(ch, True).wait_send()
        pl.when(is0)(lambda: half(ch).wait_send())
        for at in range(4):
            got(r_die.at[at, ch], grid.at[2 * at + 1, ch])
            got(s_die.at[at, ch], grid.at[2 * at + 1, ch])
        for slot in range(3):
            got(s_z.at[slot, ch], grid.at[0, ch])

    each(CHAN, settle)

    def settle_down(i):
        @pl.when(is0)
        def _():
            got(s_y.at[1, i], grid.at[0, i])
            pl.when(turned_down(i))(lambda: got(s_z.at[3, i], grid.at[0, i]))

        @pl.when(is1)
        def _():
            got(s_y.at[0, i], grid.at[0, i])
            got(s_y.at[0, i + HALF], grid.at[0, i])
            pl.when(i >= len(TURNED_DOWN))(lambda: got(s_y.at[1, i], grid.at[0, i]))

    each(HALF, settle_down)
    got(s_auto, autos.at[pl.ds(0, COLS - 1)])
    got(s_inv, inv.at[pl.ds(1, 8)])
    got(r_inv, inv.at[pl.ds(1, 8)])


def tile_kernel(grid, inv, inv_t, out):
    h = pl.program_id(0)
    own = grid[0, 0]
    turned = jnp.concatenate([own[:, BLOCK:], -own[:, :BLOCK]], axis=1)
    lanes = lax.broadcasted_iota(jnp.int32, (BLOCK, CHAN), 1)
    rows = jnp.sum(jnp.where(lanes == h, inv_t[...], 0.0), axis=1, keepdims=True) * (1.0 / BLOCK)
    for k in range(9):
        partner = grid[k, 0]
        factor = rows * inv[k, pl.ds(h, 1), :]
        for half, left in enumerate((own, turned)):
            gram = lax.dot_general(left, partner, (((1,), (1,)), ((), ())), preferred_element_type=jnp.float32)
            out[0, k, :, half * BLOCK:(half + 1) * BLOCK] = (gram * factor).astype(jnp.bfloat16)


def per_device(voltages, auto_prev, station_order):
    x = jnp.transpose(voltages.reshape(PIECE, 64, WIDE), (1, 0, 2))
    order = station_order.reshape(COLS, BLOCK)
    any_space = pl.BlockSpec(memory_space=pl.ANY)
    vmem = pl.BlockSpec(memory_space=pltpu.VMEM)
    dma = pltpu.SemaphoreType.DMA
    grid, inv, inv_t = pl.pallas_call(
        comm_kernel,
        out_shape=(
            jax.ShapeDtypeStruct((9, CHAN, 4, 2, PIECE, WIDE), jnp.bfloat16),
            jax.ShapeDtypeStruct((9, CHAN, BLOCK), jnp.float32),
            jax.ShapeDtypeStruct((BLOCK, CHAN), jnp.float32),
        ),
        in_specs=[any_space, vmem, vmem],
        out_specs=(any_space, vmem, vmem),
        scratch_shapes=[
            pltpu.VMEM((HALF, 4, 2, PIECE, WIDE), jnp.bfloat16),
            pltpu.VMEM((CHAN, 4, PIECE, WIDE), jnp.bfloat16),
            pltpu.VMEM((COLS, CHAN, BLOCK), jnp.float32),
            dma((CHAN,)), dma((CHAN,)), dma((CHAN,)), dma((CHAN,)), dma((4, CHAN)), dma((2, CHAN)), dma((4, CHAN)), dma, dma,
            dma((CHAN,)), dma((CHAN,)), dma((CHAN,)), dma((4, CHAN)), dma((HALF,)), dma((4, CHAN)), dma, dma,
        ],
        compiler_params=pltpu.CompilerParams(collective_id=0, has_side_effects=True, vmem_limit_bytes=8*2**20),
    )(x, auto_prev, order)
    grid = grid.reshape(9, CHAN, BLOCK, WIDE)
    return pl.pallas_call(
        tile_kernel,
        grid=(CHAN,),
        out_shape=jax.ShapeDtypeStruct((CHAN, 9, BLOCK, WIDE), jnp.bfloat16),
        in_specs=[
            pl.BlockSpec((9, 1, BLOCK, WIDE), lambda h: (0, h, 0, 0)),
            vmem,
            vmem,
        ],
        out_specs=pl.BlockSpec((1, 9, BLOCK, WIDE), lambda h: (h, 0, 0, 0)),compiler_params=pltpu.CompilerParams(vmem_limit_bytes=12*2**20),
    )(grid, inv, inv_t)


def solution(mesh):
    return jax.shard_map(
        per_device,
        mesh=mesh,
        in_specs=(P(("col", "row"), None, None, None), P("row", "col"), P()),
        out_specs=P("row", None, "col", None),
        check_vma=False,
    )
```

```python
import functools

import jax
import jax.numpy as jnp
from jax import lax
from jax.experimental import pallas as pl
from jax.experimental.pallas import tpu as pltpu
from jax.sharding import PartitionSpec as P

CHAN = 8
HALF = CHAN // 2
PIECE = 32
BLOCK = 256
WIDE = 512
COLS = 16
TURNED_DOWN = (0, 1)
AHEAD = 2.0
FIRST, RATE = 9.0, 3.4
UNIT, DELAY = 5.8, 3.0
INVERT = 26.0
HALVES = 20.0


def plan():
    hops, at = {}, {}
    for n in range(CHAN):
        ch = n // 2 + HALF * (n % 2)
        falls = ch < HALF
        z = "down" if falls else "up"
        for y in (0, 1):
            at["row", ch, y] = FIRST + RATE * n
            hops["relay", ch, y] = ("y", UNIT / 2, [("row", ch, y)])
            hops["near", ch, y] = (z, UNIT / 2, [("row", ch, y)])
            hops["far", ch, y] = (z, UNIT / 2, [("relay", ch, 1 - y)])
            first = [("near", ch, y), ("far", ch, y)]
            if falls:
                hops["64", ch, y] = (z, UNIT, first)
                hops["42", ch, y] = (z, UNIT, [("64", ch, y)])
            else:
                hops["24", ch, y] = (z, UNIT, first)
                hops["13", ch, y] = (z, UNIT, [("y21", ch, 1)] if y == 0 else [("half", ch, 0)])
        hops["half", ch, 0] = ("y", UNIT / 2, [("row", ch, 0)])
        if falls:
            hops["y23", ch, 0] = ("y", UNIT, [("42", ch, 0)])
            hops["y43", ch, 1] = ("y", UNIT, [("64", ch, 1)])
            if ch in TURNED_DOWN:
                hops["31", ch, 0] = (z, UNIT, [("y43", ch, 1)])
            else:
                hops["y21", ch, 1] = ("y", UNIT, [("42", ch, 1)])
        else:
            hops["y21", ch, 1] = ("y", UNIT, [("near", ch, 1), ("far", ch, 1)])
    after = {}
    for name, (_, _, needs) in hops.items():
        for need in needs:
            after.setdefault(need, []).append(name)
    tail = {}

    def left(name):
        if name not in tail:
            tail[name] = hops[name][1] + DELAY + max([left(n) for n in after.get(name, [])], default=0.0)
        return tail[name]

    free, events, waiting = {}, ([], []), dict(hops)
    while waiting:
        best = None
        for name, (link, _, needs) in waiting.items():
            if all(need in at for need in needs):
                ready = max([at[need] for need in needs] + [HALVES if name[0] == "half" else 0.0])
                start = max(ready, free.get((link, name[2]), 0.0))
                key = (round(start, 3), -round(left(name), 3), name)
                if best is None or key < best[0]:
                    best = (key, name, ready, start)
        _, name, ready, start = best
        link, takes, _ = waiting.pop(name)
        free[link, name[2]] = start + takes
        at[name] = start + takes + DELAY
        events[name[2]].append((max(ready, start - AHEAD), name[0], name[1]))
    arrives = {}
    for ch in range(CHAN):
        for y in (0, 1):
            falls = ch < HALF
            arrives[0, ch, y] = at["relay", ch, 1 - y]
            if falls:
                arrives[4, ch, y] = at["64", ch, y]
                arrives[2, ch, y] = at["42", ch, y]
                arrives[3, ch, y] = at["y43", ch, 1] if y == 0 else at["y23", ch, 0]
                turned = ("31", ch, 0) if ch in TURNED_DOWN else ("y21", ch, 1)
                arrives[1, ch, y] = at[turned] if y == 0 else at["half", ch, 0]
            else:
                arrives[2, ch, y] = max(at["near", ch, y], at["far", ch, y])
                arrives[4, ch, y] = at["24", ch, y]
                arrives[3, ch, y] = at["13", ch, y]
                arrives[1, ch, y] = at["y21", ch, 1] if y == 0 else at["half", ch, 0]
            for j in range(1, 5):
                events[y].append((arrives[j, ch, y], "arrived", (j, ch)))
    return tuple(sorted(e, key=lambda item: (item[0], item[1], str(item[2]))) for e in events), arrives


def scaled(own, partner, factor):
    turned = jnp.concatenate([own[:, BLOCK:], -own[:, :BLOCK]], axis=1)
    grams = [
        lax.dot_general(left, partner, (((1,), (1,)), ((), ())), preferred_element_type=jnp.float32)
        for left in (own, turned)
    ]
    return [(gram * factor).astype(jnp.bfloat16) for gram in grams]


def row_factor(inv_t, h):
    lanes = lax.broadcasted_iota(jnp.int32, (BLOCK, CHAN), 1)
    return jnp.sum(jnp.where(lanes == h, inv_t[...], 0.0), axis=1, keepdims=True) * (1.0 / BLOCK)


def comm_kernel(
    x, auto, order, grid, inv, inv_t, ups, downs,
    transit, relay, autos,
    bar_local, s_a2a, s_relay, s_half, s_z, s_y, s_die, s_auto, s_inv,
    r_x, r_o, r_rel, r_blk, r_trans, r_die, r_auto, r_inv,
):
    row = lax.axis_index("row")
    col = lax.axis_index("col")
    xpos, yhi = row // 2, row % 2
    core, ylo = col % 2, (col // 2) % 2
    sib = col + 1 - 2 * core
    ynb = col + 2 - 4 * ylo
    up = (col + 4) % COLS
    down = (col + COLS - 4) % COLS
    is0, is1 = ylo == 0, ylo == 1
    other = 1 - yhi

    def peer_x(d):
        return ((xpos + d) % 4) * 2 + yhi

    def peer_o(d):
        return ((xpos + d) % 4) * 2 + other

    def remote(src, dst, ss, rs, **where):
        return pltpu.make_async_remote_copy(
            src_ref=src, dst_ref=dst, send_sem=ss, recv_sem=rs,
            device_id=where, device_id_type=pl.DeviceIdType.MESH,
        )

    barrier = pltpu.get_barrier_semaphore()
    for d in range(1, 4):
        pl.semaphore_signal(barrier, inc=1, device_id={"row": peer_x(d), "col": col}, device_id_type=pl.DeviceIdType.MESH)
    for d in range(4):
        pl.semaphore_signal(barrier, inc=1, device_id={"row": peer_o(d), "col": ynb}, device_id_type=pl.DeviceIdType.MESH)
    for d in range(1, COLS):
        pl.semaphore_signal(barrier, inc=1, device_id={"row": row, "col": (col + d) % COLS}, device_id_type=pl.DeviceIdType.MESH)
    pl.semaphore_wait(barrier, 3 + 4 + COLS - 1)

    def local_own(ch):
        return pltpu.make_async_copy(x.at[row * CHAN + ch], grid.at[0, ch, xpos, yhi], bar_local.at[ch])

    def a2a_x(ch, d):
        return remote(x.at[peer_x(d) * CHAN + ch], grid.at[0, ch, xpos, yhi], s_a2a.at[ch], r_x.at[ch],
                      row=peer_x(d), col=col)

    def a2a_o(ch, d, first):
        dst = grid.at[2, ch, xpos, yhi] if first else relay.at[ch, xpos]
        return remote(x.at[peer_o(d) * CHAN + ch], dst, s_a2a.at[ch], r_o.at[ch], row=peer_o(d), col=ynb)

    def relayed(ch, first):
        src = relay.at[ch] if first else grid.at[2, ch, :, other]
        return remote(src, grid.at[0, ch, :, other], s_relay.at[ch], r_rel.at[ch], row=row, col=ynb)

    def half(ch):
        return remote(grid.at[0, ch, :, yhi], grid.at[2, ch, :, yhi], s_half.at[ch], r_blk.at[0, ch], row=row, col=ynb)

    def z_send(ch, j, to, target, slot):
        src = transit.at[ch] if j == 6 else grid.at[2 * j, ch]
        if to == 6:
            return remote(src, transit.at[ch], s_z.at[slot, ch], r_trans.at[ch], row=row, col=target)
        return remote(src, grid.at[2 * to, ch], s_z.at[slot, ch], r_blk.at[to - 1, ch], row=row, col=target)

    def y_send(ch, j, to, slot):
        return remote(grid.at[2 * j, ch], grid.at[2 * to, ch], s_y.at[slot, ch], r_blk.at[to - 1, ch], row=row, col=ynb)

    def die(ch, j):
        at = j - core
        return remote(grid.at[2 * j, ch], grid.at[2 * at + 1, ch], s_die.at[at, ch], r_die.at[at, ch], row=row, col=sib)

    def die_start(ch, j):
        if j == 0:
            pl.when(core == 0)(lambda: die(ch, j).start())
        elif j == 4:
            pl.when(core == 1)(lambda: die(ch, j).start())
        else:
            die(ch, j).start()

    def got(sem, ref):
        pltpu.make_async_copy(ref, ref, sem).wait()

    def got_block(j, ch):
        got(r_blk.at[j - 1, ch], grid.at[2 * j, ch])

    def each(count, body):
        lax.fori_loop(0, count, lambda i, carry: (body(i), carry)[1], 0)

    def send_auto(d):
        return remote(auto, autos.at[col], s_auto, r_auto, row=row, col=(col + d) % COLS)

    def exchange(ch):
        local_own(ch).start()
        for d in range(1, 4):
            a2a_x(ch, d).start()
        for d in range(4):
            pl.when(is0)(lambda: a2a_o(ch, d, True).start())
            pl.when(is1)(lambda: a2a_o(ch, d, False).start())

    exchange(0)
    exchange(HALF)
    each(COLS - 1, lambda i: send_auto(i + 1).start())
    autos[pl.ds(col, 1)] = auto[...][None]

    def exchange_pair(i):
        exchange(i + 1)
        exchange(i + 1 + HALF)

    each(HALF - 1, exchange_pair)

    def gathered(b, total):
        mine = order[pl.ds(col, 1), :]
        values = autos[pl.ds(b, 1)].reshape(CHAN, BLOCK)
        high = values.astype(jnp.bfloat16)
        rest = values - high.astype(jnp.float32)
        mid = rest.astype(jnp.bfloat16)
        low = (rest - mid.astype(jnp.float32)).astype(jnp.bfloat16)
        stations = lax.broadcasted_iota(jnp.int32, (BLOCK, BLOCK), 0) + b * BLOCK
        hot = jnp.where(stations == mine, 1.0, 0.0).astype(jnp.bfloat16)
        for part in (low, mid, high):
            total = total + jnp.dot(part, hot, preferred_element_type=jnp.float32)
        return total

    def invert():
        got(r_auto, autos.at[pl.ds(0, COLS - 1)])
        values = lax.fori_loop(0, COLS, gathered, jnp.zeros((CHAN, BLOCK), jnp.float32))
        inverse = 1.0 / jnp.sqrt(values)
        inv[0] = inverse
        inv_t[...] = jnp.transpose(inverse)

    def send_inv(k):
        return remote(inv.at[0], inv.at[k], s_inv, r_inv, row=row, col=(col + k) % COLS)

    def pass_on():
        for k in range(1, 9):
            send_inv(k).start()

    def take_inv():
        got(r_inv, inv.at[pl.ds(1, 8)])

    def own_z(ch, part):
        src = grid.at[0, ch, :, part]
        if ch < HALF:
            return remote(src, transit.at[ch, :, part], s_z.at[0, ch], r_trans.at[ch], row=row, col=down)
        return remote(src, grid.at[4, ch, :, part], s_z.at[0, ch], r_blk.at[1, ch], row=row, col=up)

    seen = (set(), set())

    def once(y, *what):
        if what in seen[y]:
            return False
        seen[y].add(what)
        return True

    def need(y, j, ch):
        if not once(y, "block", j, ch):
            return
        if j == 1 and y == 1:
            need_far(y, ch)
            got(r_blk.at[0, ch], relay.at[ch])
        else:
            got_block(j, ch)
        die_start(ch, j)

    def need_near(y, ch):
        if once(y, "near", ch):
            local_own(ch).wait()
            got(r_x.at[ch], x.at[pl.ds(0, 3)])

    def need_far(y, ch):
        if once(y, "far", ch):
            got(r_o.at[ch], relay.at[ch])

    def need_own(y, ch):
        need_near(y, ch)
        if once(y, "own", ch):
            got(r_rel.at[ch], relay.at[ch])
            die_start(ch, 0)

    def run(y, what, ch):
        if what == "arrived":
            need(y, *ch)
        elif what == "relay":
            need_far(y, ch)
            relayed(ch, y == 0).start()
        elif what == "near":
            need_near(y, ch)
            own_z(ch, yhi).start()
        elif what == "far":
            need_own(y, ch)
            own_z(ch, other).start()
        elif what == "half":
            need_near(y, ch)
            half(ch).start()
        elif what == "64":
            got(r_trans.at[ch], transit.at[ch])
            z_send(ch, 6, 4, down, 1).start()
        elif what in ("42", "24", "13", "31"):
            j, to = int(what[0]), int(what[1])
            need(y, j, ch)
            slot = {"42": 2, "24": 1, "13": 2, "31": 3}[what]
            z_send(ch, j, to, down if ch < HALF else up, slot).start()
        else:
            j, to = int(what[1]), int(what[2])
            need(y, j, ch)
            y_send(ch, j, to, 1 if what == "y23" or (what == "y21" and ch < HALF) else 0).start()

    events, arrives = plan()
    done = [0, 0]

    def until(time, blocks=()):
        for y in (0, 1):
            @pl.when(ylo == y)
            def _(y=y):
                while done[y] < len(events[y]) and events[y][done[y]][0] < time:
                    run(y, *events[y][done[y]][1:])
                    done[y] += 1
                for j, ch in blocks:
                    need_own(y, ch)
                    if j > 0:
                        need(y, j, ch)

    def tiles(first, k):
        def one(i):
            ch = first + i
            if k % 2 == 1:
                got(r_die.at[k // 2, ch], grid.at[k, ch])
            own = grid[0, ch].reshape(BLOCK, WIDE)
            factor = row_factor(inv_t, ch) * inv[k, pl.ds(ch, 1), :]
            for part, value in enumerate(scaled(own, grid[k, ch].reshape(BLOCK, WIDE), factor)):
                lanes = slice(part * BLOCK, (part + 1) * BLOCK)
                if first == 0:
                    downs[i, k // 8, :, lanes] = value
                else:
                    ups[i, k, :, lanes] = value

        each(HALF, one)

    def when_ready(first, k):
        from_blocks = [k // 2] if k % 2 == 0 else [k // 2, k // 2 + 1]
        latest = max(arrives[j, first + i, y] for j in from_blocks for i in range(HALF) for y in (0, 1))
        return latest + (3.0 if k % 2 == 1 else 0.0)

    until(INVERT)
    invert()
    until(INVERT + 2.0)
    pass_on()
    jobs = sorted([(when_ready(HALF, k), HALF, k) for k in range(9)] + [(when_ready(0, k), 0, k) for k in (0, 8)])
    time = INVERT + 6.0
    for index, (ready, first, k) in enumerate(jobs):
        time = max(time, ready)
        until(time, [(k // 2 if k % 2 == 0 else 0, first + i) for i in range(HALF)])
        if index == 0:
            take_inv()
        tiles(first, k)
        time += 1.0
    until(1e9)

    def settle(ch):
        got(s_a2a.at[ch], x.at[pl.ds(0, 7)])
        relayed(ch, True).wait_send()
        pl.when(is0)(lambda: half(ch).wait_send())
        for at in range(4):
            got(s_die.at[at, ch], grid.at[2 * at + 1, ch])
        for slot in range(3):
            got(s_z.at[slot, ch], grid.at[0, ch])

    each(CHAN, settle)

    def settle_down(i):
        @pl.when(is0)
        def _():
            got(s_y.at[1, i], grid.at[0, i])
            pl.when(i < len(TURNED_DOWN))(lambda: got(s_z.at[3, i], grid.at[0, i]))

        @pl.when(is1)
        def _():
            got(s_y.at[0, i], grid.at[0, i])
            got(s_y.at[0, i + HALF], grid.at[0, i])
            pl.when(i >= len(TURNED_DOWN))(lambda: got(s_y.at[1, i], grid.at[0, i]))

        for at in range(4):
            got(r_die.at[at, i], grid.at[2 * at + 1, i])

    each(HALF, settle_down)
    got(s_auto, autos.at[pl.ds(0, COLS - 1)])
    got(s_inv, inv.at[pl.ds(1, 8)])


def finish_kernel(grid, inv, inv_t, ups, downs, out, late, s_up, s_down, s_late):
    copies = [pltpu.make_async_copy(ups.at[i], out.at[HALF + i], s_up.at[i]) for i in range(HALF)]
    for i in range(HALF):
        for at in range(2):
            copies.append(pltpu.make_async_copy(downs.at[i, at], out.at[i, 8 * at], s_down.at[i, at]))
    for copy in copies:
        copy.start()

    def one(ch, carry):
        rows = row_factor(inv_t, ch)
        own = grid[0, ch]
        for k in range(1, 8):
            factor = rows * inv[k, pl.ds(ch, 1), :]
            for part, value in enumerate(scaled(own, grid[k, ch], factor)):
                late[ch, k - 1, :, part * BLOCK:(part + 1) * BLOCK] = value
            pltpu.make_async_copy(late.at[ch, k - 1], out.at[ch, k], s_late.at[ch, k - 1]).start()
        return carry

    lax.fori_loop(0, HALF, one, 0)
    for copy in copies:
        copy.wait()

    def wait(ch, carry):
        for k in range(1, 8):
            pltpu.make_async_copy(late.at[ch, k - 1], out.at[ch, k], s_late.at[ch, k - 1]).wait()
        return carry

    lax.fori_loop(0, HALF, wait, 0)


def per_device(voltages, auto_prev, station_order):
    x = jnp.transpose(voltages.reshape(PIECE, 64, WIDE), (1, 0, 2))
    order = station_order.reshape(COLS, BLOCK)
    any_space = pl.BlockSpec(memory_space=pl.ANY)
    vmem = pl.BlockSpec(memory_space=pltpu.VMEM)
    dma = pltpu.SemaphoreType.DMA
    grid, inv, inv_t, ups, downs = pl.pallas_call(
        comm_kernel,
        out_shape=(
            jax.ShapeDtypeStruct((9, CHAN, 4, 2, PIECE, WIDE), jnp.bfloat16),
            jax.ShapeDtypeStruct((9, CHAN, BLOCK), jnp.float32),
            jax.ShapeDtypeStruct((BLOCK, CHAN), jnp.float32),
            jax.ShapeDtypeStruct((HALF, 9, BLOCK, WIDE), jnp.bfloat16),
            jax.ShapeDtypeStruct((HALF, 2, BLOCK, WIDE), jnp.bfloat16),
        ),
        in_specs=[any_space, vmem, vmem],
        out_specs=(vmem, vmem, vmem, vmem, vmem),
        scratch_shapes=[
            pltpu.VMEM((HALF, 4, 2, PIECE, WIDE), jnp.bfloat16),
            pltpu.VMEM((CHAN, 4, PIECE, WIDE), jnp.bfloat16),
            pltpu.VMEM((COLS, CHAN, BLOCK), jnp.float32),
            dma((CHAN,)), dma((CHAN,)), dma((CHAN,)), dma((CHAN,)), dma((4, CHAN)), dma((2, CHAN)), dma((4, CHAN)), dma, dma,
            dma((CHAN,)), dma((CHAN,)), dma((CHAN,)), dma((4, CHAN)), dma((HALF,)), dma((4, CHAN)), dma, dma,
        ],
        compiler_params=pltpu.CompilerParams(collective_id=0, has_side_effects=True, vmem_limit_bytes=8*2**20),
    )(x, auto_prev, order)
    grid = grid.reshape(9, CHAN, BLOCK, WIDE)
    return pl.pallas_call(
        finish_kernel,
        out_shape=jax.ShapeDtypeStruct((CHAN, 9, BLOCK, WIDE), jnp.bfloat16),
        in_specs=[vmem] * 5,
        out_specs=any_space,
        scratch_shapes=[
            pltpu.VMEM((HALF, 7, BLOCK, WIDE), jnp.bfloat16),
            dma((HALF,)), dma((HALF, 2)), dma((HALF, 7)),
        ],
        compiler_params=pltpu.CompilerParams(vmem_limit_bytes=12 * 2**20),
    )(grid, inv, inv_t, ups, downs)


def solution(mesh):
    return jax.shard_map(
        per_device,
        mesh=mesh,
        in_specs=(P(("col", "row"), None, None, None), P("row", "col"), P()),
        out_specs=P("row", None, "col", None),
        check_vma=False,
    )
```

```python
import heapq

import jax
import jax.numpy as jnp
from jax import lax
from jax.experimental import pallas as pl
from jax.experimental.pallas import tpu as pltpu
from jax.sharding import PartitionSpec as P

CHAN = 8
EARLY = 5
PIECE = 32
BLOCK = 256
WIDE = 512
COLS = 16
AHEAD = 3.0
FIRST, RATE = 8.0, 3.8
UNIT, DELAY = 2.88, 3.3
DEPTH = 3
INVERT = 26.0
SLOTS = 13
UP, DOWN, ACROSS = 1, 2, 3
TREES = (
    (
        (6, 9, 15, 18, 26),
        (7, 10, 13, 18, 26),
        (6, 10, 15, 18, 26),
        (7, 10, 15, 18, 26),
        (7, 9, 13, 17),
        (7, 11, 13, 17),
        (7, 10, 15, 18, 26),
        (7, 10, 13, 18, 26),
    ),
    (
        (3, 11, 13, 17),
        (3, 11, 13, 17),
        (3, 9, 13, 17),
        (2, 11, 13, 17),
        (3, 9, 13, 17),
        (2, 10, 13, 19, 21),
        (2, 11, 13, 17),
        (3, 11, 13, 17),
    ),
    (
        (11, 13, 19, 22, 30),
        (10, 15, 19, 22, 30),
        (11, 14, 17, 22, 30),
        (11, 13, 17, 22, 30),
        (10, 13, 19, 21),
        (11, 13, 19, 21),
        (11, 13, 17, 21),
        (10, 14, 19, 22, 30),
    ),
    (
        (7, 9, 15, 17, 23),
        (6, 9, 15, 17, 21),
        (7, 9, 15, 17, 23),
        (7, 10, 13, 19, 21),
        (6, 9, 15, 17, 23),
        (7, 10, 13, 19, 22, 30),
        (6, 9, 15, 17, 21),
        (7, 11, 14, 19, 22, 30),
    ),
)


def offset(kind, node):
    return node - (1 if kind >= 2 else 0)


def kept(kind, node):
    return 0 <= offset(kind, node) <= 4


def comes_from(node, link):
    if link == ACROSS:
        return node // 2 * 2 + 1 - node % 2
    step = 6 if link == UP else 2
    return (node + step) % 8


def plan():
    roots = (0, 1, 1, 0)
    children, left = {}, {}
    for kind in range(4):
        for ch in range(CHAN):
            for code in TREES[kind][ch]:
                node, link = code // 4, code % 4
                children.setdefault((kind, ch, comes_from(node, link)), []).append((node, link))

    def rest(kind, ch, node):
        return UNIT + DELAY + max([rest(kind, ch, n) for n, _ in children.get((kind, ch, node), [])], default=0.0)

    queue, busy, heap, at, events = {}, {}, [], {}, ([], [])
    count = 0
    for kind in range(4):
        for ch in range(CHAN):
            heapq.heappush(heap, (FIRST + RATE * ch, count, None, (kind, ch, roots[kind])))
            count += 1
    while heap:
        now, _, line, what = heapq.heappop(heap)
        lines = [line] if line else []
        if what:
            kind, ch, node = what
            at[what] = now
            for to, link in children.get(what, []):
                line = (node % 2, link)
                heapq.heappush(queue.setdefault(line, []), (-rest(kind, ch, to) + DEPTH * ch, count, now, (kind, ch, node, link, to)))
                count += 1
                lines.append(line)
        for line in lines:
            if busy.get(line, 0.0) <= now + 1e-6 and queue.get(line):
                _, _, ready, hop = heapq.heappop(queue[line])
                events[line[0]].append((max(ready, now - AHEAD), count, hop))
                busy[line] = now + UNIT
                heapq.heappush(heap, (now + UNIT + DELAY, count, None, (hop[0], hop[1], hop[4])))
                heapq.heappush(heap, (now + UNIT, count + 1, line, None))
                count += 2
    for (kind, ch, node), time in at.items():
        if kept(kind, node):
            count += 1
            events[node % 2].append((time, count, (kind, ch, node)))
    return tuple(sorted(e) for e in events), at


def scaled(own, partner, factor):
    turned = jnp.concatenate([own[:, BLOCK:], -own[:, :BLOCK]], axis=1)
    grams = [
        lax.dot_general(left, partner, (((1,), (1,)), ((), ())), preferred_element_type=jnp.float32)
        for left in (own, turned)
    ]
    return [(gram * factor).astype(jnp.bfloat16) for gram in grams]


def row_factor(inv_t, h):
    lanes = lax.broadcasted_iota(jnp.int32, (BLOCK, CHAN), 1)
    return jnp.sum(jnp.where(lanes == h, inv_t[...], 0.0), axis=1, keepdims=True) * (1.0 / BLOCK)


def comm_kernel(
    x, auto, order, grid, inv, inv_t, ready_tiles,
    transit, autos, placed,
    s_local, s_a2a, s_hop, s_die, s_auto, s_inv,
    r_x, r_o, r_blk, r_transit, r_die, r_auto, r_inv,
):
    row = lax.axis_index("row")
    col = lax.axis_index("col")
    xpos, yhi = row // 2, row % 2
    core, ylo = col % 2, (col // 2) % 2
    sib = col + 1 - 2 * core
    ynb = col + 2 - 4 * ylo
    up = (col + 4) % COLS
    down = (col + COLS - 4) % COLS
    is0, is1 = ylo == 0, ylo == 1
    other = 1 - yhi

    def peer_x(d):
        return ((xpos + d) % 4) * 2 + yhi

    def peer_o(d):
        return ((xpos + d) % 4) * 2 + other

    def remote(src, dst, ss, rs, **where):
        return pltpu.make_async_remote_copy(
            src_ref=src, dst_ref=dst, send_sem=ss, recv_sem=rs,
            device_id=where, device_id_type=pl.DeviceIdType.MESH,
        )

    barrier = pltpu.get_barrier_semaphore()
    for d in range(1, 4):
        pl.semaphore_signal(barrier, inc=1, device_id={"row": peer_x(d), "col": col}, device_id_type=pl.DeviceIdType.MESH)
    for d in range(4):
        pl.semaphore_signal(barrier, inc=1, device_id={"row": peer_o(d), "col": ynb}, device_id_type=pl.DeviceIdType.MESH)
    for d in range(1, COLS):
        pl.semaphore_signal(barrier, inc=1, device_id={"row": row, "col": (col + d) % COLS}, device_id_type=pl.DeviceIdType.MESH)
    pl.semaphore_wait(barrier, 3 + 4 + COLS - 1)

    parts = (yhi, other)

    def local_own(ch):
        return pltpu.make_async_copy(x.at[row * CHAN + ch], grid.at[0, ch, xpos, yhi], s_local.at[ch])

    def a2a_x(ch, d):
        return remote(x.at[peer_x(d) * CHAN + ch], grid.at[0, ch, xpos, yhi], s_a2a.at[ch], r_x.at[ch],
                      row=peer_x(d), col=col)

    def a2a_o(ch, d, first):
        dst = grid.at[2, ch, xpos, yhi] if first else transit.at[1, ch, xpos, yhi]
        return remote(x.at[peer_o(d) * CHAN + ch], dst, s_a2a.at[ch], r_o.at[ch], row=peer_o(d), col=ynb)

    def place(kind, ch, node):
        if kept(kind, node):
            return grid.at[2 * offset(kind, node), ch, :, parts[kind % 2]]
        return transit.at[kind // 2, ch, :, parts[kind % 2]]

    def arrival(kind, ch, node):
        if kept(kind, node):
            return r_blk.at[kind % 2, offset(kind, node), ch]
        return r_transit.at[kind // 2, kind % 2, ch]

    def hop(kind, ch, node, link, to, slot):
        where = {"row": row, "col": {UP: up, DOWN: down, ACROSS: ynb}[link]}
        return remote(place(kind, ch, node), place(kind, ch, to), s_hop.at[slot, ch], arrival(kind, ch, to), **where)

    def die(ch, j, part):
        at = j - core
        return remote(grid.at[2 * j, ch, :, part], grid.at[2 * at + 1, ch, :, part], s_die.at[at, ch], r_die.at[at, ch],
                      row=row, col=sib)

    def die_start(ch, j, part):
        if j == 0:
            pl.when(core == 0)(lambda: die(ch, j, part).start())
        elif j == 4:
            pl.when(core == 1)(lambda: die(ch, j, part).start())
        else:
            die(ch, j, part).start()

    def got(sem, ref):
        pltpu.make_async_copy(ref, ref, sem).wait()

    def each(count, body):
        lax.fori_loop(0, count, lambda i, carry: (body(i), carry)[1], 0)

    def send_auto(d):
        return remote(auto, autos.at[col], s_auto, r_auto, row=row, col=(col + d) % COLS)

    def exchange(ch):
        local_own(ch).start()
        for d in range(1, 4):
            a2a_x(ch, d).start()
        for d in range(4):
            pl.when(is0)(lambda: a2a_o(ch, d, True).start())
            pl.when(is1)(lambda: a2a_o(ch, d, False).start())

    exchange(0)
    each(COLS - 1, lambda i: send_auto(i + 1).start())
    own_auto = pltpu.make_async_copy(auto, autos.at[col], s_local.at[CHAN])
    own_auto.start()
    own_order = pltpu.make_async_copy(order, placed, s_local.at[CHAN + 1])
    own_order.start()

    each(CHAN - 1, lambda i: exchange(i + 1))

    def gathered(b, total):
        mine = placed[pl.ds(pl.multiple_of(col * BLOCK, BLOCK), BLOCK)].reshape(1, BLOCK)
        values = autos[pl.ds(b, 1)].reshape(CHAN, BLOCK)
        high = values.astype(jnp.bfloat16)
        rest = values - high.astype(jnp.float32)
        mid = rest.astype(jnp.bfloat16)
        low = (rest - mid.astype(jnp.float32)).astype(jnp.bfloat16)
        stations = lax.broadcasted_iota(jnp.int32, (BLOCK, BLOCK), 0) + b * BLOCK
        hot = jnp.where(stations == mine, 1.0, 0.0).astype(jnp.bfloat16)
        for part in (low, mid, high):
            total = total + jnp.dot(part, hot, preferred_element_type=jnp.float32)
        return total

    def invert():
        got(r_auto, autos.at[pl.ds(0, COLS - 1)])
        own_auto.wait()
        own_order.wait()
        values = lax.fori_loop(0, COLS, gathered, jnp.zeros((CHAN, BLOCK), jnp.float32))
        inverse = 1.0 / jnp.sqrt(values)
        inv[0] = inverse
        inv_t[...] = jnp.transpose(inverse)

    def send_inv(k):
        return remote(inv.at[0], inv.at[k], s_inv, r_inv, row=row, col=(col + k) % COLS)

    def pass_on():
        for k in range(1, 9):
            send_inv(k).start()

    def take_inv():
        got(r_inv, inv.at[pl.ds(1, 8)])

    events, arrives = plan()
    seen, done, sent = (set(), set()), [0, 0], ([], [])

    def need(y, kind, ch, node):
        if (kind, ch, node) in seen[y]:
            return
        seen[y].add((kind, ch, node))
        part = parts[kind % 2]
        if kind == (0, 2)[y] and node == y:
            local_own(ch).wait()
            got(r_x.at[ch], x.at[pl.ds(0, 3)])
        elif kind == (3, 1)[y] and node == y:
            got(r_o.at[ch], transit.at[0, ch, :, 0])
        else:
            got(arrival(kind, ch, node), transit.at[0, ch, :, 0])
        if kept(kind, node):
            die_start(ch, offset(kind, node), part)

    def until(time, channel=None):
        for y in (0, 1):
            @pl.when(ylo == y)
            def _(y=y):
                while done[y] < len(events[y]) and events[y][done[y]][0] < time:
                    what = events[y][done[y]][2]
                    done[y] += 1
                    need(y, *what[:3])
                    if len(what) > 3:
                        slot = len([ch for ch, _ in sent[y] if ch == what[1]])
                        sent[y].append((what[1], slot))
                        hop(*what, slot).start()
                if channel is not None:
                    for kind, ch, node in sorted(arrives):
                        if ch == channel and node % 2 == y and kept(kind, node):
                            need(y, kind, ch, node)

    def tiles(ch, first, count):
        own = grid[0, ch].reshape(BLOCK, WIDE)
        rows = row_factor(inv_t, ch)

        def one(i):
            k = first + i
            factor = rows * inv[k, ch:ch + 1, :]
            for part, value in enumerate(scaled(own, grid[k, ch].reshape(BLOCK, WIDE), factor)):
                ready_tiles[ch, k, :, part * BLOCK:(part + 1) * BLOCK] = value

        each(count, one)

    until(INVERT)
    invert()
    until(INVERT + 2.0)
    pass_on()
    time = INVERT + 6.0
    for ch in range(EARLY):
        time = max(time, 3.0 + max(t for (kind, c, node), t in arrives.items() if c == ch and kept(kind, node)))
        until(time, ch)
        if ch == 0:
            take_inv()
        for at in range(4):
            got(r_die.at[at, ch], grid.at[2 * at + 1, ch])
        for first in (0, 3, 6):
            until(time)
            tiles(ch, first, 3)
            time += 0.7
    until(1e9)

    def settle(ch):
        got(s_a2a.at[ch], x.at[pl.ds(0, 7)])
        for at in range(4):
            got(s_die.at[at, ch], grid.at[2 * at + 1, ch])

    each(CHAN, settle)
    for ch in range(EARLY, CHAN):
        for at in range(4):
            got(r_die.at[at, ch], grid.at[2 * at + 1, ch])
    for y in (0, 1):
        @pl.when(ylo == y)
        def _(y=y):
            for ch, slot in sent[y]:
                got(s_hop.at[slot, ch], transit.at[0, ch, :, 0])
    got(s_auto, autos.at[pl.ds(0, COLS - 1)])
    got(s_inv, inv.at[pl.ds(1, 8)])


def finish_kernel(grid, inv, inv_t, ready_tiles, out, late, s_ready, s_late):
    copies = [pltpu.make_async_copy(ready_tiles.at[i], out.at[i], s_ready.at[i]) for i in range(EARLY)]
    for copy in copies:
        copy.start()

    def write(i, k):
        return pltpu.make_async_copy(late.at[i, k], out.at[EARLY + i, k], s_late.at[i, k])

    def one(i, carry):
        rows = row_factor(inv_t, EARLY + i)
        own = grid[0, EARLY + i]
        for k in range(9):
            factor = rows * inv[k, pl.ds(EARLY + i, 1), :]
            for part, value in enumerate(scaled(own, grid[k, EARLY + i], factor)):
                late[i, k, :, part * BLOCK:(part + 1) * BLOCK] = value
            write(i, k).start()
        return carry

    lax.fori_loop(0, CHAN - EARLY, one, 0)
    for copy in copies:
        copy.wait()

    def wait(i, carry):
        for k in range(9):
            write(i, k).wait()
        return carry

    lax.fori_loop(0, CHAN - EARLY, wait, 0)


def per_device(voltages, auto_prev, station_order):
    x = jnp.transpose(voltages.reshape(PIECE, 64, WIDE), (1, 0, 2))
    in_hbm = pl.BlockSpec(memory_space=pltpu.HBM)
    any_space = pl.BlockSpec(memory_space=pl.ANY)
    vmem = pl.BlockSpec(memory_space=pltpu.VMEM)
    dma = pltpu.SemaphoreType.DMA
    grid, inv, inv_t, ready_tiles = pl.pallas_call(
        comm_kernel,
        out_shape=(
            jax.ShapeDtypeStruct((9, CHAN, 4, 2, PIECE, WIDE), jnp.bfloat16),
            jax.ShapeDtypeStruct((9, CHAN, BLOCK), jnp.float32),
            jax.ShapeDtypeStruct((BLOCK, CHAN), jnp.float32),
            jax.ShapeDtypeStruct((EARLY, 9, BLOCK, WIDE), jnp.bfloat16),
        ),
        in_specs=[any_space, in_hbm, in_hbm],
        out_specs=(vmem, vmem, vmem, vmem),
        scratch_shapes=[
            pltpu.VMEM((2, CHAN, 4, 2, PIECE, WIDE), jnp.bfloat16),
            pltpu.VMEM((COLS, CHAN, BLOCK), jnp.float32),
            pltpu.VMEM((COLS * BLOCK,), jnp.int32),
            dma((CHAN + 2,)), dma((CHAN,)), dma((SLOTS, CHAN)), dma((4, CHAN)), dma, dma,
            dma((CHAN,)), dma((CHAN,)), dma((2, 5, CHAN)), dma((2, 2, CHAN)), dma((4, CHAN)), dma, dma,
        ],
        compiler_params=pltpu.CompilerParams(collective_id=0, has_side_effects=True, vmem_limit_bytes=10 * 2**20),
    )(x, *(pltpu.with_memory_space_constraint(a, pltpu.HBM) for a in (auto_prev, station_order)))
    grid = grid.reshape(9, CHAN, BLOCK, WIDE)
    return pl.pallas_call(
        finish_kernel,
        out_shape=jax.ShapeDtypeStruct((CHAN, 9, BLOCK, WIDE), jnp.bfloat16),
        in_specs=[vmem] * 4,
        out_specs=any_space,
        scratch_shapes=[
            pltpu.VMEM((CHAN - EARLY, 9, BLOCK, WIDE), jnp.bfloat16),
            dma((EARLY,)), dma((CHAN - EARLY, 9)),
        ],
        compiler_params=pltpu.CompilerParams(vmem_limit_bytes=12 * 2**20),
    )(grid, inv, inv_t, ready_tiles)


def solution(mesh):
    return jax.shard_map(
        per_device,
        mesh=mesh,
        in_specs=(P(("col", "row"), None, None, None), P("row", "col"), P()),
        out_specs=P("row", None, "col", None),
        check_vma=False,
    )
```

```python
import heapq

import jax
import jax.numpy as jnp
from jax import lax
from jax.experimental import pallas as pl
from jax.experimental.pallas import tpu as pltpu
from jax.sharding import PartitionSpec as P

CHAN = 8
EARLY = 4
PIECE = 32
BLOCK = 256
WIDE = 512
COLS = 16
AHEAD = 3.0
FIRST, RATE = 8.0, 3.8
UNIT, DELAY = 2.88, 3.3
DEPTH = 3
INVERT = 26.0
SLOTS = 13
UP, DOWN, ACROSS = 1, 2, 3
TREES = (
    (
        (6, 9, 15, 18, 26),
        (7, 10, 13, 18, 26),
        (6, 10, 15, 18, 26),
        (7, 10, 15, 18, 26),
        (7, 9, 13, 17),
        (7, 11, 13, 17),
        (7, 10, 15, 18, 26),
        (7, 10, 13, 18, 26),
    ),
    (
        (3, 11, 13, 17),
        (3, 11, 13, 17),
        (3, 9, 13, 17),
        (2, 11, 13, 17),
        (3, 9, 13, 17),
        (2, 10, 13, 19, 21),
        (2, 11, 13, 17),
        (3, 11, 13, 17),
    ),
    (
        (11, 13, 19, 22, 30),
        (10, 15, 19, 22, 30),
        (11, 14, 17, 22, 30),
        (11, 13, 17, 22, 30),
        (10, 13, 19, 21),
        (11, 13, 19, 21),
        (11, 13, 17, 21),
        (10, 14, 19, 22, 30),
    ),
    (
        (7, 9, 15, 17, 23),
        (6, 9, 15, 17, 21),
        (7, 9, 15, 17, 23),
        (7, 10, 13, 19, 21),
        (6, 9, 15, 17, 23),
        (7, 10, 13, 19, 22, 30),
        (6, 9, 15, 17, 21),
        (7, 11, 14, 19, 22, 30),
    ),
)


def offset(kind, node):
    return node - (1 if kind >= 2 else 0)


def kept(kind, node):
    return 0 <= offset(kind, node) <= 4


def comes_from(node, link):
    if link == ACROSS:
        return node // 2 * 2 + 1 - node % 2
    step = 6 if link == UP else 2
    return (node + step) % 8


def plan():
    roots = (0, 1, 1, 0)
    children, left = {}, {}
    for kind in range(4):
        for ch in range(CHAN):
            for code in TREES[kind][ch]:
                node, link = code // 4, code % 4
                children.setdefault((kind, ch, comes_from(node, link)), []).append((node, link))

    def rest(kind, ch, node):
        return UNIT + DELAY + max([rest(kind, ch, n) for n, _ in children.get((kind, ch, node), [])], default=0.0)

    queue, busy, heap, at, events = {}, {}, [], {}, ([], [])
    count = 0
    for kind in range(4):
        for ch in range(CHAN):
            heapq.heappush(heap, (FIRST + RATE * ch, count, None, (kind, ch, roots[kind])))
            count += 1
    while heap:
        now, _, line, what = heapq.heappop(heap)
        lines = [line] if line else []
        if what:
            kind, ch, node = what
            at[what] = now
            for to, link in children.get(what, []):
                line = (node % 2, link)
                heapq.heappush(queue.setdefault(line, []), (-rest(kind, ch, to) + DEPTH * ch, count, now, (kind, ch, node, link, to)))
                count += 1
                lines.append(line)
        for line in lines:
            if busy.get(line, 0.0) <= now + 1e-6 and queue.get(line):
                _, _, ready, hop = heapq.heappop(queue[line])
                events[line[0]].append((max(ready, now - AHEAD), count, hop))
                busy[line] = now + UNIT
                heapq.heappush(heap, (now + UNIT + DELAY, count, None, (hop[0], hop[1], hop[4])))
                heapq.heappush(heap, (now + UNIT, count + 1, line, None))
                count += 2
    for (kind, ch, node), time in at.items():
        if kept(kind, node):
            count += 1
            events[node % 2].append((time, count, (kind, ch, node)))
    return tuple(sorted(e) for e in events), at


def scaled(own, partner, factor):
    turned = jnp.concatenate([own[:, BLOCK:], -own[:, :BLOCK]], axis=1)
    grams = [
        lax.dot_general(left, partner, (((1,), (1,)), ((), ())), preferred_element_type=jnp.float32)
        for left in (own, turned)
    ]
    return [(gram * factor).astype(jnp.bfloat16) for gram in grams]


def row_factor(inv_t, h):
    lanes = lax.broadcasted_iota(jnp.int32, (BLOCK, CHAN), 1)
    return jnp.sum(jnp.where(lanes == h, inv_t[...], 0.0), axis=1, keepdims=True) * (1.0 / BLOCK)


def comm_kernel(
    x, auto, order, grid, inv, inv_t, ready_tiles,
    transit, autos, placed,
    s_local, s_a2a, s_hop, s_die, s_auto, s_inv,
    r_x, r_o, r_blk, r_transit, r_die, r_auto, r_inv,
):
    row = lax.axis_index("row")
    col = lax.axis_index("col")
    xpos, yhi = row // 2, row % 2
    core, ylo = col % 2, (col // 2) % 2
    sib = col + 1 - 2 * core
    ynb = col + 2 - 4 * ylo
    up = (col + 4) % COLS
    down = (col + COLS - 4) % COLS
    is0, is1 = ylo == 0, ylo == 1
    other = 1 - yhi

    def peer_x(d):
        return ((xpos + d) % 4) * 2 + yhi

    def peer_o(d):
        return ((xpos + d) % 4) * 2 + other

    def remote(src, dst, ss, rs, **where):
        return pltpu.make_async_remote_copy(
            src_ref=src, dst_ref=dst, send_sem=ss, recv_sem=rs,
            device_id=where, device_id_type=pl.DeviceIdType.MESH,
        )

    barrier = pltpu.get_barrier_semaphore()
    for d in range(1, 4):
        pl.semaphore_signal(barrier, inc=1, device_id={"row": peer_x(d), "col": col}, device_id_type=pl.DeviceIdType.MESH)
    for d in range(4):
        pl.semaphore_signal(barrier, inc=1, device_id={"row": peer_o(d), "col": ynb}, device_id_type=pl.DeviceIdType.MESH)
    for d in range(1, COLS):
        pl.semaphore_signal(barrier, inc=1, device_id={"row": row, "col": (col + d) % COLS}, device_id_type=pl.DeviceIdType.MESH)
    pl.semaphore_wait(barrier, 3 + 4 + COLS - 1)

    parts = (yhi, other)

    def local_own(ch):
        return pltpu.make_async_copy(x.at[row * CHAN + ch], grid.at[0, ch, xpos, yhi], s_local.at[ch])

    def a2a_x(ch, d):
        return remote(x.at[peer_x(d) * CHAN + ch], grid.at[0, ch, xpos, yhi], s_a2a.at[ch], r_x.at[ch],
                      row=peer_x(d), col=col)

    def a2a_o(ch, d, first):
        dst = grid.at[2, ch, xpos, yhi] if first else transit.at[1, ch, xpos, yhi]
        return remote(x.at[peer_o(d) * CHAN + ch], dst, s_a2a.at[ch], r_o.at[ch], row=peer_o(d), col=ynb)

    def place(kind, ch, node):
        if kept(kind, node):
            return grid.at[2 * offset(kind, node), ch, :, parts[kind % 2]]
        return transit.at[kind // 2, ch, :, parts[kind % 2]]

    def arrival(kind, ch, node):
        if kept(kind, node):
            return r_blk.at[kind % 2, offset(kind, node), ch]
        return r_transit.at[kind // 2, kind % 2, ch]

    def hop(kind, ch, node, link, to, slot):
        where = {"row": row, "col": {UP: up, DOWN: down, ACROSS: ynb}[link]}
        return remote(place(kind, ch, node), place(kind, ch, to), s_hop.at[slot, ch], arrival(kind, ch, to), **where)

    def die(ch, j, part):
        at = j - core
        return remote(grid.at[2 * j, ch, :, part], grid.at[2 * at + 1, ch, :, part], s_die.at[at, ch], r_die.at[at, ch],
                      row=row, col=sib)

    def die_start(ch, j, part):
        if j == 0:
            pl.when(core == 0)(lambda: die(ch, j, part).start())
        elif j == 4:
            pl.when(core == 1)(lambda: die(ch, j, part).start())
        else:
            die(ch, j, part).start()

    def got(sem, ref):
        pltpu.make_async_copy(ref, ref, sem).wait()

    def each(count, body):
        lax.fori_loop(0, count, lambda i, carry: (body(i), carry)[1], 0)

    def send_auto(d):
        return remote(auto, autos.at[col], s_auto, r_auto, row=row, col=(col + d) % COLS)

    def exchange(ch):
        local_own(ch).start()
        for d in range(1, 4):
            a2a_x(ch, d).start()
        for d in range(4):
            pl.when(is0)(lambda: a2a_o(ch, d, True).start())
            pl.when(is1)(lambda: a2a_o(ch, d, False).start())

    exchange(0)
    each(COLS - 1, lambda i: send_auto(i + 1).start())
    own_auto = pltpu.make_async_copy(auto, autos.at[col], s_local.at[CHAN])
    own_auto.start()
    own_order = pltpu.make_async_copy(order, placed, s_local.at[CHAN + 1])
    own_order.start()

    each(CHAN - 1, lambda i: exchange(i + 1))

    def gathered(b, total):
        mine = placed[pl.ds(pl.multiple_of(col * BLOCK, BLOCK), BLOCK)].reshape(1, BLOCK)
        values = autos[pl.ds(b, 1)].reshape(CHAN, BLOCK)
        high = values.astype(jnp.bfloat16)
        rest = values - high.astype(jnp.float32)
        mid = rest.astype(jnp.bfloat16)
        low = (rest - mid.astype(jnp.float32)).astype(jnp.bfloat16)
        stations = lax.broadcasted_iota(jnp.int32, (BLOCK, BLOCK), 0) + b * BLOCK
        hot = jnp.where(stations == mine, 1.0, 0.0).astype(jnp.bfloat16)
        for part in (low, mid, high):
            total = total + jnp.dot(part, hot, preferred_element_type=jnp.float32)
        return total

    def invert():
        got(r_auto, autos.at[pl.ds(0, COLS - 1)])
        own_auto.wait()
        own_order.wait()
        values = lax.fori_loop(0, COLS, gathered, jnp.zeros((CHAN, BLOCK), jnp.float32))
        inverse = 1.0 / jnp.sqrt(values)
        inv[0] = inverse
        inv_t[...] = jnp.transpose(inverse)

    def send_inv(k):
        return remote(inv.at[0], inv.at[k], s_inv, r_inv, row=row, col=(col + k) % COLS)

    def pass_on():
        for k in range(1, 9):
            send_inv(k).start()

    def take_inv():
        got(r_inv, inv.at[pl.ds(1, 8)])

    events, arrives = plan()
    seen, done, sent = (set(), set()), [0, 0], ([], [])

    def need(y, kind, ch, node):
        if (kind, ch, node) in seen[y]:
            return
        seen[y].add((kind, ch, node))
        part = parts[kind % 2]
        if kind == (0, 2)[y] and node == y:
            local_own(ch).wait()
            got(r_x.at[ch], x.at[pl.ds(0, 3)])
        elif kind == (3, 1)[y] and node == y:
            got(r_o.at[ch], transit.at[0, ch, :, 0])
        else:
            got(arrival(kind, ch, node), transit.at[0, ch, :, 0])
        if kept(kind, node):
            die_start(ch, offset(kind, node), part)

    def until(time, channel=None):
        for y in (0, 1):
            @pl.when(ylo == y)
            def _(y=y):
                while done[y] < len(events[y]) and events[y][done[y]][0] < time:
                    what = events[y][done[y]][2]
                    done[y] += 1
                    need(y, *what[:3])
                    if len(what) > 3:
                        slot = len([ch for ch, _ in sent[y] if ch == what[1]])
                        sent[y].append((what[1], slot))
                        hop(*what, slot).start()
                if channel is not None:
                    for kind, ch, node in sorted(arrives):
                        if ch == channel and node % 2 == y and kept(kind, node):
                            need(y, kind, ch, node)

    def tiles(ch, first, count):
        own = grid[0, ch].reshape(BLOCK, WIDE)
        rows = row_factor(inv_t, ch)

        def one(i):
            k = first + i
            factor = rows * inv[k, ch:ch + 1, :]
            for part, value in enumerate(scaled(own, grid[k, ch].reshape(BLOCK, WIDE), factor)):
                ready_tiles[ch, k, :, part * BLOCK:(part + 1) * BLOCK] = value

        each(count, one)

    until(INVERT)
    invert()
    until(INVERT + 2.0)
    pass_on()
    time = INVERT + 6.0
    for ch in range(EARLY):
        time = max(time, 3.0 + max(t for (kind, c, node), t in arrives.items() if c == ch and kept(kind, node)))
        until(time, ch)
        if ch == 0:
            take_inv()
        for at in range(4):
            got(r_die.at[at, ch], grid.at[2 * at + 1, ch])
        for first in (0, 3, 6):
            until(time)
            tiles(ch, first, 3)
            time += 0.7
    until(1e9)

    def settle(ch):
        got(s_a2a.at[ch], x.at[pl.ds(0, 7)])
        for at in range(4):
            got(s_die.at[at, ch], grid.at[2 * at + 1, ch])

    each(CHAN, settle)
    for ch in range(EARLY, CHAN):
        for at in range(4):
            got(r_die.at[at, ch], grid.at[2 * at + 1, ch])
    for y in (0, 1):
        @pl.when(ylo == y)
        def _(y=y):
            for ch, slot in sent[y]:
                got(s_hop.at[slot, ch], transit.at[0, ch, :, 0])
    got(s_auto, autos.at[pl.ds(0, COLS - 1)])
    got(s_inv, inv.at[pl.ds(1, 8)])


def finish_kernel(grid, inv, inv_t, ready_tiles, out, late, s_ready, s_late):
    copies = [pltpu.make_async_copy(ready_tiles.at[i], out.at[i], s_ready.at[i]) for i in range(EARLY)]
    for copy in copies:
        copy.start()

    def write(i, k):
        return pltpu.make_async_copy(late.at[i, k], out.at[EARLY + i, k], s_late.at[i, k])

    def one(i, carry):
        rows = row_factor(inv_t, EARLY + i)
        own = grid[0, EARLY + i]
        for k in range(9):
            factor = rows * inv[k, pl.ds(EARLY + i, 1), :]
            for part, value in enumerate(scaled(own, grid[k, EARLY + i], factor)):
                late[i, k, :, part * BLOCK:(part + 1) * BLOCK] = value
            write(i, k).start()
        return carry

    lax.fori_loop(0, CHAN - EARLY, one, 0)
    for copy in copies:
        copy.wait()

    def wait(i, carry):
        for k in range(9):
            write(i, k).wait()
        return carry

    lax.fori_loop(0, CHAN - EARLY, wait, 0)


def per_device(voltages, auto_prev, station_order):
    x = jnp.transpose(voltages.reshape(PIECE, 64, WIDE), (1, 0, 2))
    in_hbm = pl.BlockSpec(memory_space=pltpu.HBM)
    any_space = pl.BlockSpec(memory_space=pl.ANY)
    vmem = pl.BlockSpec(memory_space=pltpu.VMEM)
    dma = pltpu.SemaphoreType.DMA
    grid, inv, inv_t, ready_tiles = pl.pallas_call(
        comm_kernel,
        out_shape=(
            jax.ShapeDtypeStruct((9, CHAN, 4, 2, PIECE, WIDE), jnp.bfloat16),
            jax.ShapeDtypeStruct((9, CHAN, BLOCK), jnp.float32),
            jax.ShapeDtypeStruct((BLOCK, CHAN), jnp.float32),
            jax.ShapeDtypeStruct((EARLY, 9, BLOCK, WIDE), jnp.bfloat16),
        ),
        in_specs=[any_space, in_hbm, in_hbm],
        out_specs=(vmem, vmem, vmem, vmem),
        scratch_shapes=[
            pltpu.VMEM((2, CHAN, 4, 2, PIECE, WIDE), jnp.bfloat16),
            pltpu.VMEM((COLS, CHAN, BLOCK), jnp.float32),
            pltpu.VMEM((COLS * BLOCK,), jnp.int32),
            dma((CHAN + 2,)), dma((CHAN,)), dma((SLOTS, CHAN)), dma((4, CHAN)), dma, dma,
            dma((CHAN,)), dma((CHAN,)), dma((2, 5, CHAN)), dma((2, 2, CHAN)), dma((4, CHAN)), dma, dma,
        ],
        compiler_params=pltpu.CompilerParams(collective_id=0, has_side_effects=True, vmem_limit_bytes=10 * 2**20),
    )(x, *(pltpu.with_memory_space_constraint(a, pltpu.HBM) for a in (auto_prev, station_order)))
    grid = grid.reshape(9, CHAN, BLOCK, WIDE)
    return pl.pallas_call(
        finish_kernel,
        out_shape=jax.ShapeDtypeStruct((CHAN, 9, BLOCK, WIDE), jnp.bfloat16),
        in_specs=[vmem] * 4,
        out_specs=any_space,
        scratch_shapes=[
            pltpu.VMEM((CHAN - EARLY, 9, BLOCK, WIDE), jnp.bfloat16),
            dma((EARLY,)), dma((CHAN - EARLY, 9)),
        ],
        compiler_params=pltpu.CompilerParams(vmem_limit_bytes=12 * 2**20),
    )(grid, inv, inv_t, ready_tiles)


def solution(mesh):
    return jax.shard_map(
        per_device,
        mesh=mesh,
        in_specs=(P(("col", "row"), None, None, None), P("row", "col"), P()),
        out_specs=P("row", None, "col", None),
        check_vma=False,
    )
```
